32 devices in a mesh: row: 16 (over z, x, core), col: 2 (over y).
Axes of the slice: x: 2, y: 2, z: 4, core: 2. Of those that a mesh axis runs over, the one named last changes fastest.
Arguments:
- pivots: int32 [256], replicated, may hold values from 0 to 4095, as said below
- panel: float32 [4096, 256], P(('row', 'col')), may hold values from -6 to 6
- prior: bfloat16 [4096, 3072], P(('row', 'col')), may hold values from -0.796875 to 0.796875
- finished: bfloat16 [4096, 256], P(('row', 'col')), may hold values from -6 to 6
- pairs: int32 [4096], replicated, may hold values from 0 to 639999, as said below
- occupied: bfloat16 [800, 120], replicated, may hold values from -0.21875 to 0.21875
Outputs:
- updated: float32 [4096, 256], P(('row', 'col'))
- halves: float32 [256, 120, 800], P(('row', 'col'))
The draws below stay inside these ranges and needn't reach their ends.
Inputs may be any that keep to these rules, and one draw needn't show every extreme that they name: `pivots`: distinct rows; at most 16 of them lie among the rows of one device (aligned blocks of 128 rows), and one device holds exactly 16. `pairs`: each value a * 800 + b with 0 <= b <= a < 800; all distinct and increasing.
All inputs are finite; a program needn't handle non-finite values.
Results may differ from the reference program's by a relative error of at most 0.0003.
Values may be sent and summed in bfloat16 or wider, within the bound.
A program may use at most 64 MiB of HBM per device.

```python
import jax
import jax.numpy as jnp
from jax import lax

K = 3072
PIVOTS = 256
NAO = 800
NOCC = 120
ROWS_DEV = 128
PAIRS = 4096
PIV_MOST = 16
DEVICES = 32


def draw_pivots(key, part):
    key_full, key_score, key_offset, key_shuffle = jax.random.split(jax.random.fold_in(key, 11), 4)
    total_slots = DEVICES * PIV_MOST
    full_block = jax.random.randint(key_full, (), 0, DEVICES)
    slot_ids = jnp.arange(total_slots, dtype=jnp.int32)
    scores = jax.random.permutation(key_score, total_slots).astype(jnp.int32)
    scores = jnp.where(slot_ids // PIV_MOST == full_block, -1 - slot_ids % PIV_MOST, scores)
    ordering = jnp.argsort(scores, stable=True)
    chosen = ordering[:PIVOTS].astype(jnp.int32)
    spacing = ROWS_DEV // PIV_MOST
    offsets = chosen % PIV_MOST * spacing + jax.random.randint(key_offset, (PIVOTS,), 0, spacing)
    result = chosen // PIV_MOST * ROWS_DEV + offsets
    return jax.random.permutation(key_shuffle, result).astype(jnp.int32)


def draw_pairs(key, part):
    total = NAO * (NAO + 1) // 2
    picked = jax.random.permutation(jax.random.fold_in(key, 23), total)[:PAIRS].astype(jnp.int32)
    picked = jnp.sort(picked)
    counter = jnp.arange(NAO, dtype=jnp.int32)
    starts = counter * (counter + 1) // 2
    first_ao = jnp.searchsorted(starts[1:], picked, side='right').astype(jnp.int32)
    second_ao = picked - jnp.take(starts, first_ao)
    return (first_ao * NAO + second_ao).astype(jnp.int32)


def block_scale(stream_key, dims, pieces, low, largest):
    def one(dim, blocks):
        steps = jax.random.uniform(jax.random.fold_in(jax.random.fold_in(stream_key, 6), dim), (blocks,), jnp.float32, low / len(pieces), largest / len(pieces))
        return jnp.repeat(jnp.exp(steps), dims[dim] // blocks).reshape((-1,) + (1,) * (len(dims) - dim - 1))

    factor_of = one(*pieces[0])
    for cut in pieces[1:]:
        factor_of = factor_of * one(*cut)
    return factor_of


def normal_values(own_key, extent, deviation, most, cuts=(), kind=jnp.bfloat16):
    values = jax.random.normal(own_key, extent, jnp.float32) * deviation
    if len(cuts) > 0:
        values = block_scale(own_key, extent, cuts, -0.22, 0.18) * values
    return jnp.clip(values, min=-most, max=most).astype(kind)


def setup_inputs(seed: int = 0) -> dict:
    seeds = jax.random.split(jax.random.key(seed), 7)
    pivots = draw_pivots(jax.random.fold_in(seeds[6], 71), 0)
    panel = normal_values(seeds[1], (PAIRS, PIVOTS), 1.0, 6.0, ((0, 32),), jnp.float32)
    prior = normal_values(seeds[2], (PAIRS, K), 0.134, 0.796875, ((0, 32),))
    finished = normal_values(seeds[3], (PAIRS, PIVOTS), 1.0, 6.0, ((0, 32),))
    pairs = draw_pairs(jax.random.fold_in(seeds[6], 71), 0)
    occupied = normal_values(seeds[5], (NAO, NOCC), NAO ** -0.5, 0.21875)
    return dict(pivots=pivots, panel=panel, prior=prior, finished=finished, pairs=pairs, occupied=occupied)


def build_matrix(column, pair_ids, mirrored, off_diag):
    matrix = jnp.zeros((NAO * NAO,), jnp.bfloat16)
    matrix = matrix.at[pair_ids].add(column)
    matrix = matrix.at[mirrored].add(jnp.where(off_diag, column, jnp.zeros_like(column)))
    return matrix.reshape(NAO, NAO)


def reference(pivots, panel, prior, finished, pairs, occupied):
    pivot_rows = jnp.take(prior, pivots, axis=0)
    updated = panel - jnp.dot(prior, pivot_rows.T, preferred_element_type=jnp.float32)
    first_ao = pairs // NAO
    second_ao = pairs % NAO
    mirrored = (second_ao * NAO + first_ao).astype(jnp.int32)
    off_diag = first_ao != second_ao

    def one_vector(column):
        matrix = build_matrix(column, pairs, mirrored, off_diag)
        return jnp.dot(occupied.T, matrix, preferred_element_type=jnp.float32)

    halves = lax.map(one_vector, finished.T)
    return updated, halves
```

```python
import functools

import jax
import jax.numpy as jnp
from jax import lax
from jax.experimental import pallas as pl
from jax.experimental.pallas import tpu as pltpu
from jax.sharding import PartitionSpec as P

MESH = pl.DeviceIdType.MESH
LANES = 128
SUBL = 8


def exchange_kernel(
    row_count, col_count, depth,
    target_ref, fin_ref, slot_ref,
    rfin_ref, gat_ref,
    rslot, slot_send, slot_recv, fin_send, fin_recv,
    ag_recv, z_send, plane_send, core_send,
):
    devices = row_count * col_count
    r = lax.axis_index("row")
    c = lax.axis_index("col")
    me = r * col_count + c
    xs = 2
    zs = row_count // (2 * xs)
    core = r % 2
    x = (r // 2) % xs
    z = r // (2 * xs)

    def row_of(zz, xx, kk):
        return (zz * xs + xx) * 2 + kk

    def block_of(zz, xx, kk, yy):
        return row_of(zz, xx, kk) * col_count + yy

    barrier = pltpu.get_barrier_semaphore()

    def greet(k, carry):
        peer = (me + k) % devices
        pl.semaphore_signal(
            barrier, inc=1, device_id=(peer // col_count, peer % col_count), device_id_type=MESH
        )
        return carry

    lax.fori_loop(1, devices, greet, 0)
    pl.semaphore_wait(barrier, devices - 1)

    def slot_copy(peer, source):
        return pltpu.make_async_remote_copy(
            src_ref=slot_ref.at[peer], dst_ref=rslot.at[source],
            send_sem=slot_send.at[peer], recv_sem=slot_recv.at[source],
            device_id=(peer // col_count, peer % col_count), device_id_type=MESH,
        )

    def fin_copy(peer, source):
        return pltpu.make_async_remote_copy(
            src_ref=fin_ref.at[peer], dst_ref=rfin_ref.at[source],
            send_sem=fin_send.at[peer], recv_sem=fin_recv.at[source],
            device_id=(peer // col_count, peer % col_count), device_id_type=MESH,
        )

    def send_slot(k, carry):
        slot_copy((me + k) % devices, me).start()
        return carry

    def send_fin(k, carry):
        fin_copy((me + k) % devices, me).start()
        return carry

    lax.fori_loop(1, devices, send_slot, 0)
    lax.fori_loop(1, devices, send_fin, 0)
    rslot[me] = slot_ref[me]
    rfin_ref[me] = fin_ref[me]
    slot_total = rslot.shape[0] * rslot.shape[1]
    pivots = target_ref.shape[1]
    rows = lax.broadcasted_iota(jnp.int32, (slot_total, pivots), 0)
    one_hot = jnp.where(rows == target_ref[...], 1.0, 0.0).astype(jnp.bfloat16)

    def take_slot(k, carry):
        peer = (me + k) % devices
        slot_copy(peer, peer).wait_recv()
        return carry

    lax.fori_loop(1, devices, take_slot, 0)
    packed = lax.dot_general(
        rslot[...].reshape(slot_total, LANES), one_hot, (((0,), (0,)), ((), ())),
        preferred_element_type=jnp.float32,
    )
    gat_ref[me] = packed[:depth].astype(jnp.bfloat16)

    def block_copy(block, send_sem, zz, xx, kk, yy):
        return pltpu.make_async_remote_copy(
            src_ref=gat_ref.at[block], dst_ref=gat_ref.at[block],
            send_sem=send_sem, recv_sem=ag_recv.at[block],
            device_id=(row_of(zz, xx, kk), yy), device_id_type=MESH,
        )

    started = []

    def go(copy):
        copy.start()
        started.append(copy)

    plane = [(dx, dy) for dx in range(xs) for dy in range(col_count)]
    for dz in range(1, zs):
        go(block_copy(me, z_send.at[dz], (z + dz) % zs, x, core, c))
    for dz in range(zs):
        zz = (z + zs - dz) % zs
        block = block_of(zz, x, core, c)
        if dz > 0:
            block_copy(block, z_send.at[0], z, x, core, c).wait_recv()
        for dx, dy in plane[1:]:
            go(block_copy(
                block, plane_send.at[dz, dx * col_count + dy],
                z, (x + dx) % xs, core, (c + dy) % col_count,
            ))
        go(block_copy(block, core_send.at[dz, 0], z, x, 1 - core, c))
    for dz in range(zs):
        zz = (z + zs - dz) % zs
        for dx, dy in plane[1:]:
            block = block_of(zz, (x + dx) % xs, core, (c + dy) % col_count)
            block_copy(block, z_send.at[0], z, x, core, c).wait_recv()
            go(block_copy(
                block, core_send.at[dz, dx * col_count + dy], z, x, 1 - core, c
            ))

    def take_fin(k, carry):
        peer = (me + k) % devices
        fin_copy(peer, peer).wait_recv()
        fin_copy(peer, me).wait_send()
        slot_copy(peer, me).wait_send()
        return carry

    lax.fori_loop(1, devices, take_fin, 0)
    for dz in range(zs):
        zz = (z + zs - dz) % zs
        for dx, dy in plane:
            block = block_of(zz, (x + dx) % xs, 1 - core, (c + dy) % col_count)
            block_copy(block, z_send.at[0], z, x, core, c).wait_recv()
    for copy in started:
        copy.wait_send()


def exchange(mesh_shape, target, fin, slots, depth):
    row_count, col_count = mesh_shape
    devices = row_count * col_count
    zs = row_count // 4
    dma = pltpu.SemaphoreType.DMA
    vmem = pl.BlockSpec(memory_space=pltpu.VMEM)
    return pl.pallas_call(
        functools.partial(exchange_kernel, row_count, col_count, depth),
        out_shape=(
            jax.ShapeDtypeStruct(fin.shape, jnp.bfloat16),
            jax.ShapeDtypeStruct((devices, depth, target.shape[1]), jnp.bfloat16),
        ),
        in_specs=[vmem] * 3,
        out_specs=(vmem, vmem),
        scratch_shapes=[
            pltpu.VMEM(slots.shape, jnp.bfloat16),
            dma((devices,)), dma((devices,)), dma((devices,)), dma((devices,)),
            dma((devices,)), dma((zs,)), dma((zs, 2 * col_count)), dma((zs, 2 * col_count)),
        ],
        compiler_params=pltpu.CompilerParams(
            collective_id=0, has_side_effects=True, vmem_limit_bytes=40 * 1024 * 1024
        ),
        name="exchange",
    )(target, fin, slots)


def halves_kernel(orbitals, tiles, lower_ref, upper_ref, fin_ref, occ_ref, out_ref, mat):
    v = pl.program_id(0)
    stripe = orbitals * SUBL

    @pl.when(v == 0)
    def _():
        zero = jnp.zeros((40 * SUBL, LANES), jnp.float32)

        def clear(k, carry):
            mat[pl.ds(pl.multiple_of(k * 40 * SUBL, 8), 40 * SUBL), :] = zero
            return carry

        lax.fori_loop(0, tiles * orbitals // 40, clear, 0)
        lane = lax.broadcasted_iota(jnp.int32, (SUBL, LANES), 1)

        def spread(chunk, carry):
            values = fin_ref[chunk].astype(jnp.float32)
            for j in range(LANES):
                one = jnp.broadcast_to(values[:, j : j + 1], (SUBL, LANES))
                for place in (lower_ref, upper_ref):
                    word = place[chunk * LANES + j]
                    start = pl.multiple_of((word >> 7) * SUBL, SUBL)
                    pltpu.store(
                        mat.at[pl.ds(start, SUBL), :], one, mask=lane == (word & (LANES - 1))
                    )
            return carry

        lax.fori_loop(0, fin_ref.shape[0], spread, 0)

    for t in range(0, tiles, 2):
        parts = [
            mat[pl.ds(u * stripe + v, orbitals, stride=SUBL), :].astype(jnp.bfloat16)
            for u in range(t, min(t + 2, tiles))
        ]
        block = jnp.concatenate(parts, axis=1) if len(parts) > 1 else parts[0]
        low = t * LANES
        high = min(orbitals, low + block.shape[1])
        product = jnp.dot(occ_ref[...], block, preferred_element_type=jnp.float32)
        out_ref[0, :, low:high] = product[:, : high - low]


def half_transform(received, pairs, occupied, vectors):
    orbitals, occ = occupied.shape
    tiles = pl.cdiv(orbitals, LANES)
    first = pairs // orbitals
    second = pairs % orbitals

    def place(a, b):
        return (((b >> 7) * orbitals + a) << 7) | (b & (LANES - 1))

    smem = pl.BlockSpec(memory_space=pltpu.SMEM)
    vmem = pl.BlockSpec(memory_space=pltpu.VMEM)
    return pl.pallas_call(
        functools.partial(halves_kernel, orbitals, tiles),
        grid=(vectors,),
        out_shape=jax.ShapeDtypeStruct((vectors, occ, orbitals), jnp.float32),
        in_specs=[smem, smem, vmem, vmem],
        out_specs=pl.BlockSpec((1, occ, orbitals), lambda v: (v, 0, 0)),
        scratch_shapes=[pltpu.VMEM((tiles * orbitals * SUBL, LANES), jnp.float32)],
        compiler_params=pltpu.CompilerParams(vmem_limit_bytes=48 * 1024 * 1024),
        name="halves",
    )(place(first, second), place(second, first), received, occupied.T)


def per_device(mesh_shape, pivots, panel, prior, finished, pairs, occupied):
    rows_dev, width = prior.shape
    row_count, col_count = mesh_shape
    devices = row_count * col_count
    own_index = lax.axis_index("row") * col_count + lax.axis_index("col")
    piv_count = pivots.shape[0]
    slot_cap = max(16, 2 * piv_count // devices)
    owner = pivots // rows_dev
    counter = jnp.arange(piv_count, dtype=jnp.int32)
    earlier = (counter[None, :] < counter[:, None]) & (owner[None, :] == owner[:, None])
    rank = jnp.sum(earlier, axis=1).astype(jnp.int32)
    target = owner * slot_cap + rank
    wanted = target[None, :] == (
        own_index * slot_cap + jnp.arange(slot_cap, dtype=jnp.int32)
    )[:, None]
    local = jnp.sum(jnp.where(wanted, (pivots % rows_dev)[None, :], 0), axis=1)
    select = (
        local[:, None] == jnp.arange(rows_dev, dtype=jnp.int32)[None, :]
    ).astype(jnp.bfloat16)
    slot_rows = jnp.dot(select, prior, preferred_element_type=jnp.bfloat16)
    depth = width // devices
    slots = slot_rows.reshape(slot_cap, devices, depth).transpose(1, 0, 2)
    slots = jnp.pad(slots, ((0, 0), (0, 0), (0, LANES - depth)))
    vectors = finished.shape[1] // devices
    fin = finished.T.reshape(devices, vectors, rows_dev)
    fin = jnp.pad(fin, ((0, 0), (0, SUBL - vectors), (0, 0)))
    received, gathered = exchange(mesh_shape, target[None, :], fin, slots, depth)
    halves = half_transform(received, pairs, occupied, vectors)
    updated = panel - jnp.dot(
        prior, gathered.reshape(width, piv_count), preferred_element_type=jnp.float32
    )
    return (updated, halves)


def solution(mesh):
    mesh_shape = (mesh.shape["row"], mesh.shape["col"])
    return jax.shard_map(
        functools.partial(per_device, mesh_shape),
        mesh=mesh,
        in_specs=(
            P(),
            P(("row", "col"), None),
            P(("row", "col"), None),
            P(("row", "col"), None),
            P(),
            P(),
        ),
        out_specs=(P(("row", "col"), None), P(("row", "col"), None, None)),
        check_vma=False,
    )
```

```python
import functools

import jax
import jax.numpy as jnp
from jax import lax
from jax.experimental import pallas as pl
from jax.experimental.pallas import tpu as pltpu
from jax.sharding import PartitionSpec as P

MESH = pl.DeviceIdType.MESH
LANES = 128
SUBL = 8


def exchange_kernel(
    row_count, col_count, depth,
    target_ref, local_ref, finished_ref, prior_ref,
    rfin_ref, gat_ref,
    prior_buf, fin_ref, slot_ref, rslot,
    load_sem, slot_send, slot_recv, fin_send, fin_recv,
    ag_recv, z_send, plane_send, core_send,
):
    devices = row_count * col_count
    r = lax.axis_index("row")
    c = lax.axis_index("col")
    me = r * col_count + c
    xs = 2
    zs = row_count // (2 * xs)
    core = r % 2
    x = (r // 2) % xs
    z = r // (2 * xs)

    def row_of(zz, xx, kk):
        return (zz * xs + xx) * 2 + kk

    def block_of(zz, xx, kk, yy):
        return row_of(zz, xx, kk) * col_count + yy

    def peer_of(k):
        return me ^ k if devices & (devices - 1) == 0 else (me + k) % devices

    def each_peer(body):
        if devices <= 64:
            for k in range(1, devices):
                body(peer_of(k))
        else:
            lax.fori_loop(1, devices, lambda k, carry: (body(peer_of(k)), carry)[1], 0)

    barrier = pltpu.get_barrier_semaphore()

    def greet(peer):
        pl.semaphore_signal(
            barrier, inc=1, device_id=(peer // col_count, peer % col_count), device_id_type=MESH
        )

    each_peer(greet)
    load = pltpu.make_async_copy(prior_ref, prior_buf, load_sem)
    load.start()
    target = target_ref[...]
    pivots = target.shape[1]
    slot_cap = slot_ref.shape[1]
    own_slots = me * slot_cap + lax.broadcasted_iota(jnp.int32, (slot_cap, pivots), 0)
    offsets = jnp.sum(
        jnp.where(own_slots == target, local_ref[...], 0.0), axis=1, keepdims=True
    ).astype(jnp.int32)
    rows_dev = prior_buf.shape[0]
    columns = lax.broadcasted_iota(jnp.int32, (slot_cap, rows_dev), 1)
    select = jnp.where(columns == offsets, 1.0, 0.0).astype(jnp.bfloat16)
    turned = finished_ref[...].astype(jnp.float32).T
    vectors = turned.shape[0] // devices
    if vectors < SUBL:
        fin_ref[...] = jnp.zeros_like(fin_ref)
    for d in range(devices):
        fin_ref[d, :vectors] = turned[d * vectors : (d + 1) * vectors].astype(jnp.bfloat16)
    load.wait()
    slot_rows = jnp.dot(
        select, prior_buf[...], preferred_element_type=jnp.float32
    )
    slot_ref[...] = jnp.zeros_like(slot_ref)
    for d in range(devices):
        slot_ref[d, :, :depth] = slot_rows[:, d * depth : (d + 1) * depth].astype(jnp.bfloat16)
    pl.semaphore_wait(barrier, devices - 1)

    def slot_copy(peer, source):
        return pltpu.make_async_remote_copy(
            src_ref=slot_ref.at[peer], dst_ref=rslot.at[source],
            send_sem=slot_send.at[peer], recv_sem=slot_recv.at[source],
            device_id=(peer // col_count, peer % col_count), device_id_type=MESH,
        )

    def fin_copy(peer, source):
        return pltpu.make_async_remote_copy(
            src_ref=fin_ref.at[peer], dst_ref=rfin_ref.at[source],
            send_sem=fin_send.at[peer], recv_sem=fin_recv.at[source],
            device_id=(peer // col_count, peer % col_count), device_id_type=MESH,
        )

    each_peer(lambda peer: slot_copy(peer, me).start())
    each_peer(lambda peer: fin_copy(peer, me).start())
    rslot[me] = slot_ref[me]
    rfin_ref[me] = fin_ref[me]
    slot_total = rslot.shape[0] * rslot.shape[1]
    rows = lax.broadcasted_iota(jnp.int32, (slot_total, pivots), 0)
    one_hot = jnp.where(rows == target, 1.0, 0.0).astype(jnp.bfloat16)

    each_peer(lambda peer: slot_copy(peer, peer).wait_recv())
    packed = lax.dot_general(
        rslot[...].reshape(slot_total, LANES), one_hot, (((0,), (0,)), ((), ())),
        preferred_element_type=jnp.float32,
    )
    gat_ref[me] = packed[:depth].astype(jnp.bfloat16)

    def block_copy(block, send_sem, zz, xx, kk, yy):
        return pltpu.make_async_remote_copy(
            src_ref=gat_ref.at[block], dst_ref=gat_ref.at[block],
            send_sem=send_sem, recv_sem=ag_recv.at[block],
            device_id=(row_of(zz, xx, kk), yy), device_id_type=MESH,
        )

    started = []

    def go(copy):
        copy.start()
        started.append(copy)

    plane = [(dx, dy) for dx in range(xs) for dy in range(col_count)]
    for dz in range(1, zs):
        go(block_copy(me, z_send.at[dz], (z + dz) % zs, x, core, c))
    for dz in range(zs):
        zz = (z + zs - dz) % zs
        block = block_of(zz, x, core, c)
        if dz > 0:
            block_copy(block, z_send.at[0], z, x, core, c).wait_recv()
        for dx, dy in plane[1:]:
            go(block_copy(
                block, plane_send.at[dz, dx * col_count + dy],
                z, (x + dx) % xs, core, (c + dy) % col_count,
            ))
        go(block_copy(block, core_send.at[dz, 0], z, x, 1 - core, c))
    for dz in range(zs):
        zz = (z + zs - dz) % zs
        for dx, dy in plane[1:]:
            block = block_of(zz, (x + dx) % xs, core, (c + dy) % col_count)
            block_copy(block, z_send.at[0], z, x, core, c).wait_recv()
            go(block_copy(
                block, core_send.at[dz, dx * col_count + dy], z, x, 1 - core, c
            ))

    def take_fin(peer):
        fin_copy(peer, peer).wait_recv()
        fin_copy(peer, me).wait_send()
        slot_copy(peer, me).wait_send()

    each_peer(take_fin)
    for dz in range(zs):
        zz = (z + zs - dz) % zs
        for dx, dy in plane:
            block = block_of(zz, (x + dx) % xs, 1 - core, (c + dy) % col_count)
            block_copy(block, z_send.at[0], z, x, core, c).wait_recv()
    for copy in started:
        copy.wait_send()


def exchange(mesh_shape, target, local, finished, prior, slot_cap):
    row_count, col_count = mesh_shape
    devices = row_count * col_count
    depth = prior.shape[1] // devices
    zs = row_count // 4
    dma = pltpu.SemaphoreType.DMA
    vmem = pl.BlockSpec(memory_space=pltpu.VMEM)
    fin_shape = (devices, SUBL, finished.shape[0])
    slot_shape = (devices, slot_cap, LANES)
    return pl.pallas_call(
        functools.partial(exchange_kernel, row_count, col_count, depth),
        out_shape=(
            jax.ShapeDtypeStruct(fin_shape, jnp.bfloat16),
            jax.ShapeDtypeStruct((devices, depth, target.shape[1]), jnp.bfloat16),
        ),
        in_specs=[vmem] * 3 + [pl.BlockSpec(memory_space=pl.ANY)],
        out_specs=(vmem, vmem),
        scratch_shapes=[
            pltpu.VMEM(prior.shape, jnp.bfloat16),
            pltpu.VMEM(fin_shape, jnp.bfloat16),
            pltpu.VMEM(slot_shape, jnp.bfloat16),
            pltpu.VMEM(slot_shape, jnp.bfloat16),
            dma, dma((devices,)), dma((devices,)), dma((devices,)), dma((devices,)),
            dma((devices,)), dma((zs,)), dma((zs, 2 * col_count)), dma((zs, 2 * col_count)),
        ],
        compiler_params=pltpu.CompilerParams(
            collective_id=0, has_side_effects=True, vmem_limit_bytes=40 * 1024 * 1024
        ),
        name="exchange",
    )(target, local, finished, prior)


def halves_kernel(
    orbitals, tiles, lower_ref, upper_ref, fin_ref, occ_ref, panel_ref, prior_ref, gat_ref,
    upd_ref, out_ref, mat,
):
    v = pl.program_id(0)
    stripe = orbitals * SUBL

    @pl.when(v == 0)
    def _():
        upd_ref[...] = panel_ref[...] - jnp.dot(
            prior_ref[...], gat_ref[...], preferred_element_type=jnp.float32
        )
        zero = jnp.zeros((40 * SUBL, LANES), jnp.float32)

        def clear(k, carry):
            mat[pl.ds(pl.multiple_of(k * 40 * SUBL, 8), 40 * SUBL), :] = zero
            return carry

        lax.fori_loop(0, tiles * orbitals // 40, clear, 0)
        lane = lax.broadcasted_iota(jnp.int32, (SUBL, LANES), 1)

        def spread(chunk, carry):
            values = fin_ref[chunk].astype(jnp.float32)
            for j in range(LANES):
                one = jnp.broadcast_to(values[:, j : j + 1], (SUBL, LANES))
                for place in (lower_ref, upper_ref):
                    word = place[chunk * LANES + j]
                    start = pl.multiple_of(word >> 7, SUBL)
                    here = (jnp.full((SUBL, LANES), word) & (LANES - 1)) == lane
                    pltpu.store(mat.at[pl.ds(start, SUBL), :], one, mask=here)
            return carry

        lax.fori_loop(0, fin_ref.shape[0], spread, 0)

    block = jnp.concatenate(
        [
            mat[pl.ds(t * stripe + v, orbitals, stride=SUBL), :].astype(jnp.bfloat16)
            for t in range(tiles)
        ],
        axis=1,
    )[:, :orbitals]
    out_ref[0] = jnp.dot(block, occ_ref[...], preferred_element_type=jnp.float32)


def finish(received, pairs, occupied, panel, prior, gathered, vectors):
    orbitals, occ = occupied.shape
    tiles = pl.cdiv(orbitals, LANES)
    first = pairs // orbitals
    second = pairs % orbitals

    def place(a, b):
        return (((b >> 7) * orbitals + a) << 10) | (b & (LANES - 1))

    smem = pl.BlockSpec(memory_space=pltpu.SMEM)
    vmem = pl.BlockSpec(memory_space=pltpu.VMEM)
    updated, halves = pl.pallas_call(
        functools.partial(halves_kernel, orbitals, tiles),
        grid=(vectors,),
        out_shape=(
            jax.ShapeDtypeStruct(panel.shape, jnp.float32),
            jax.ShapeDtypeStruct((vectors, orbitals, occ), jnp.float32),
        ),
        in_specs=[smem, smem] + [vmem] * 5,
        out_specs=(
            pl.BlockSpec(panel.shape, lambda v: (0, 0)),
            pl.BlockSpec((1, orbitals, occ), lambda v: (v, 0, 0)),
        ),
        scratch_shapes=[pltpu.VMEM((tiles * orbitals * SUBL, LANES), jnp.float32)],
        compiler_params=pltpu.CompilerParams(vmem_limit_bytes=48 * 1024 * 1024),
        name="halves",
    )(
        place(first, second), place(second, first), received,
        occupied, panel, prior, gathered,
    )
    return updated, halves.transpose(0, 2, 1)


def per_device(mesh_shape, pivots, panel, prior, finished, pairs, occupied):
    rows_dev, width = prior.shape
    row_count, col_count = mesh_shape
    devices = row_count * col_count
    piv_count = pivots.shape[0]
    slot_cap = max(16, 2 * piv_count // devices)
    owner = pivots // rows_dev
    counter = jnp.arange(piv_count, dtype=jnp.int32)
    earlier = (counter[None, :] < counter[:, None]) & (owner[None, :] == owner[:, None])
    rank = jnp.sum(earlier, axis=1).astype(jnp.int32)
    target = owner * slot_cap + rank
    vectors = finished.shape[1] // devices
    local = (pivots % rows_dev).astype(jnp.float32)
    received, gathered = exchange(
        mesh_shape, target[None, :], local[None, :], finished, prior, slot_cap
    )
    return finish(
        received, pairs, occupied, panel, prior, gathered.reshape(width, piv_count), vectors
    )


def solution(mesh):
    mesh_shape = (mesh.shape["row"], mesh.shape["col"])
    return jax.shard_map(
        functools.partial(per_device, mesh_shape),
        mesh=mesh,
        in_specs=(
            P(),
            P(("row", "col"), None),
            P(("row", "col"), None),
            P(("row", "col"), None),
            P(),
            P(),
        ),
        out_specs=(P(("row", "col"), None), P(("row", "col"), None, None)),
        check_vma=False,
    )
```

```python
import functools

import jax
import jax.numpy as jnp
from jax import lax
from jax.experimental import pallas as pl
from jax.experimental.pallas import tpu as pltpu
from jax.sharding import PartitionSpec as P

MESH = pl.DeviceIdType.MESH
LANES = 128
SUBL = 8


def exchange_kernel(
    row_count, col_count, depth,
    target_ref, local_ref, finished_ref, prior_ref,
    rfin_ref, gat_ref,
    prior_buf, fin_ref, slot_ref, rslot,
    load_sem, slot_send, slot_recv, fin_send, fin_recv,
    ag_recv, z_send, plane_send, core_send,
):
    devices = row_count * col_count
    r = lax.axis_index("row")
    c = lax.axis_index("col")
    me = r * col_count + c
    xs = 2
    zs = row_count // (2 * xs)
    core = r % 2
    x = (r // 2) % xs
    z = r // (2 * xs)

    def row_of(zz, xx, kk):
        return (zz * xs + xx) * 2 + kk

    def block_of(zz, xx, kk, yy):
        return row_of(zz, xx, kk) * col_count + yy

    def peer_of(k):
        return me ^ k if devices & (devices - 1) == 0 else (me + k) % devices

    def each_peer(body):
        if devices <= 64:
            for k in range(1, devices):
                body(peer_of(k))
        else:
            lax.fori_loop(1, devices, lambda k, carry: (body(peer_of(k)), carry)[1], 0)

    barrier = pltpu.get_barrier_semaphore()

    def greet(peer):
        pl.semaphore_signal(
            barrier, inc=1, device_id=(peer // col_count, peer % col_count), device_id_type=MESH
        )

    each_peer(greet)
    load = pltpu.make_async_copy(prior_ref, prior_buf, load_sem)
    load.start()
    target = target_ref[...]
    pivots = target.shape[1]
    slot_cap = slot_ref.shape[1]
    own_slots = me * slot_cap + lax.broadcasted_iota(jnp.int32, (slot_cap, pivots), 0)
    offsets = jnp.sum(
        jnp.where(own_slots == target, local_ref[...], 0.0), axis=1, keepdims=True
    ).astype(jnp.int32)
    rows_dev = prior_buf.shape[0]
    columns = lax.broadcasted_iota(jnp.int32, (slot_cap, rows_dev), 1)
    select = jnp.where(columns == offsets, 1.0, 0.0).astype(jnp.bfloat16)
    turned = finished_ref[...].astype(jnp.float32).T
    vectors = turned.shape[0] // devices
    if vectors < SUBL:
        fin_ref[...] = jnp.zeros_like(fin_ref)
    for d in range(devices):
        fin_ref[d, :vectors] = turned[d * vectors : (d + 1) * vectors].astype(jnp.bfloat16)
    load.wait()
    slot_rows = jnp.dot(
        select, prior_buf[...], preferred_element_type=jnp.float32
    )
    slot_ref[...] = jnp.zeros_like(slot_ref)
    for d in range(devices):
        slot_ref[d, :, :depth] = slot_rows[:, d * depth : (d + 1) * depth].astype(jnp.bfloat16)
    pl.semaphore_wait(barrier, devices - 1)

    def slot_copy(peer, source):
        return pltpu.make_async_remote_copy(
            src_ref=slot_ref.at[peer], dst_ref=rslot.at[source],
            send_sem=slot_send.at[peer], recv_sem=slot_recv.at[source],
            device_id=(peer // col_count, peer % col_count), device_id_type=MESH,
        )

    def fin_copy(peer, source):
        return pltpu.make_async_remote_copy(
            src_ref=fin_ref.at[peer], dst_ref=rfin_ref.at[source],
            send_sem=fin_send.at[peer], recv_sem=fin_recv.at[source],
            device_id=(peer // col_count, peer % col_count), device_id_type=MESH,
        )

    each_peer(lambda peer: slot_copy(peer, me).start())
    each_peer(lambda peer: fin_copy(peer, me).start())
    rslot[me] = slot_ref[me]
    rfin_ref[me] = fin_ref[me]
    slot_total = rslot.shape[0] * rslot.shape[1]
    rows = lax.broadcasted_iota(jnp.int32, (slot_total, pivots), 0)
    one_hot = jnp.where(rows == target, 1.0, 0.0).astype(jnp.bfloat16)

    each_peer(lambda peer: slot_copy(peer, peer).wait_recv())
    packed = lax.dot_general(
        rslot[...].reshape(slot_total, LANES), one_hot, (((0,), (0,)), ((), ())),
        preferred_element_type=jnp.float32,
    )
    gat_ref[me] = packed[:depth].astype(jnp.bfloat16)

    def block_copy(block, send_sem, zz, xx, kk, yy):
        return pltpu.make_async_remote_copy(
            src_ref=gat_ref.at[block], dst_ref=gat_ref.at[block],
            send_sem=send_sem, recv_sem=ag_recv.at[block],
            device_id=(row_of(zz, xx, kk), yy), device_id_type=MESH,
        )

    started = []

    def go(copy):
        copy.start()
        started.append(copy)

    plane = [(dx, dy) for dx in range(xs) for dy in range(col_count)]
    for dz in range(1, zs):
        go(block_copy(me, z_send.at[dz], (z + dz) % zs, x, core, c))
    for dz in range(zs):
        zz = (z + zs - dz) % zs
        block = block_of(zz, x, core, c)
        if dz > 0:
            block_copy(block, z_send.at[0], z, x, core, c).wait_recv()
        for dx, dy in plane[1:]:
            go(block_copy(
                block, plane_send.at[dz, dx * col_count + dy],
                z, (x + dx) % xs, core, (c + dy) % col_count,
            ))
        go(block_copy(block, core_send.at[dz, 0], z, x, 1 - core, c))
    for dz in range(zs):
        zz = (z + zs - dz) % zs
        for dx, dy in plane[1:]:
            block = block_of(zz, (x + dx) % xs, core, (c + dy) % col_count)
            block_copy(block, z_send.at[0], z, x, core, c).wait_recv()
            go(block_copy(
                block, core_send.at[dz, dx * col_count + dy], z, x, 1 - core, c
            ))

    def take_fin(peer):
        fin_copy(peer, peer).wait_recv()
        fin_copy(peer, me).wait_send()
        slot_copy(peer, me).wait_send()

    each_peer(take_fin)
    for dz in range(zs):
        zz = (z + zs - dz) % zs
        for dx, dy in plane:
            block = block_of(zz, (x + dx) % xs, 1 - core, (c + dy) % col_count)
            block_copy(block, z_send.at[0], z, x, core, c).wait_recv()
    for copy in started:
        copy.wait_send()


def exchange(mesh_shape, target, local, finished, prior, slot_cap):
    row_count, col_count = mesh_shape
    devices = row_count * col_count
    depth = prior.shape[1] // devices
    zs = row_count // 4
    dma = pltpu.SemaphoreType.DMA
    vmem = pl.BlockSpec(memory_space=pltpu.VMEM)
    fin_shape = (devices, SUBL, finished.shape[0])
    slot_shape = (devices, slot_cap, LANES)
    return pl.pallas_call(
        functools.partial(exchange_kernel, row_count, col_count, depth),
        out_shape=(
            jax.ShapeDtypeStruct(fin_shape, jnp.bfloat16),
            jax.ShapeDtypeStruct((devices, depth, target.shape[1]), jnp.bfloat16),
        ),
        in_specs=[vmem] * 3 + [pl.BlockSpec(memory_space=pl.ANY)],
        out_specs=(vmem, vmem),
        scratch_shapes=[
            pltpu.VMEM(prior.shape, jnp.bfloat16),
            pltpu.VMEM(fin_shape, jnp.bfloat16),
            pltpu.VMEM(slot_shape, jnp.bfloat16),
            pltpu.VMEM(slot_shape, jnp.bfloat16),
            dma, dma((devices,)), dma((devices,)), dma((devices,)), dma((devices,)),
            dma((devices,)), dma((zs,)), dma((zs, 2 * col_count)), dma((zs, 2 * col_count)),
        ],
        compiler_params=pltpu.CompilerParams(
            collective_id=0, has_side_effects=True, vmem_limit_bytes=40 * 1024 * 1024
        ),
        cost_estimate=pl.CostEstimate(flops=10**10, bytes_accessed=4 * 10**7, transcendentals=0),
        name="exchange",
    )(target, local, finished, prior)


def halves_kernel(
    orbitals, tiles, lower_ref, upper_ref, fin_ref, occ_ref, panel_ref, prior_ref, gat_ref,
    upd_ref, out_ref, mat,
):
    v = pl.program_id(0)
    stripe = orbitals * SUBL

    @pl.when(v == 0)
    def _():
        upd_ref[...] = panel_ref[...] - jnp.dot(
            prior_ref[...], gat_ref[...], preferred_element_type=jnp.float32
        )
        zero = jnp.zeros((40 * SUBL, LANES), jnp.float32)

        def clear(k, carry):
            mat[pl.ds(pl.multiple_of(k * 40 * SUBL, 8), 40 * SUBL), :] = zero
            return carry

        lax.fori_loop(0, tiles * orbitals // 40, clear, 0)
        lane = lax.broadcasted_iota(jnp.int32, (SUBL, LANES), 1)

        def spread(chunk, carry):
            values = fin_ref[chunk].astype(jnp.float32)
            for j in range(LANES):
                one = jnp.broadcast_to(values[:, j : j + 1], (SUBL, LANES))
                for place in (lower_ref, upper_ref):
                    word = place[chunk * LANES + j]
                    start = pl.multiple_of(word >> 7, SUBL)
                    here = (jnp.full((SUBL, LANES), word) & (LANES - 1)) == lane
                    pltpu.store(mat.at[pl.ds(start, SUBL), :], one, mask=here)
            return carry

        lax.fori_loop(0, fin_ref.shape[0], spread, 0)

    block = jnp.concatenate(
        [
            mat[pl.ds(t * stripe + v, orbitals, stride=SUBL), :].astype(jnp.bfloat16)
            for t in range(tiles)
        ],
        axis=1,
    )[:, :orbitals]
    out_ref[0] = jnp.dot(block, occ_ref[...], preferred_element_type=jnp.float32)


def finish(received, pairs, occupied, panel, prior, gathered, vectors):
    orbitals, occ = occupied.shape
    tiles = pl.cdiv(orbitals, LANES)
    first = pairs // orbitals
    second = pairs % orbitals

    def place(a, b):
        return (((b >> 7) * orbitals + a) << 10) | (b & (LANES - 1))

    smem = pl.BlockSpec(memory_space=pltpu.SMEM)
    vmem = pl.BlockSpec(memory_space=pltpu.VMEM)
    updated, halves = pl.pallas_call(
        functools.partial(halves_kernel, orbitals, tiles),
        grid=(vectors,),
        out_shape=(
            jax.ShapeDtypeStruct(panel.shape, jnp.float32),
            jax.ShapeDtypeStruct((vectors, orbitals, occ), jnp.float32),
        ),
        in_specs=[smem, smem] + [vmem] * 5,
        out_specs=(
            pl.BlockSpec(panel.shape, lambda v: (0, 0)),
            pl.BlockSpec((1, orbitals, occ), lambda v: (v, 0, 0)),
        ),
        scratch_shapes=[pltpu.VMEM((tiles * orbitals * SUBL, LANES), jnp.float32)],
        compiler_params=pltpu.CompilerParams(vmem_limit_bytes=48 * 1024 * 1024),
        cost_estimate=pl.CostEstimate(flops=10**10, bytes_accessed=4 * 10**7, transcendentals=0),
        name="halves",
    )(
        place(first, second), place(second, first), received,
        occupied, panel, prior, gathered,
    )
    return updated, halves.transpose(0, 2, 1)


def per_device(mesh_shape, pivots, panel, prior, finished, pairs, occupied):
    rows_dev, width = prior.shape
    row_count, col_count = mesh_shape
    devices = row_count * col_count
    piv_count = pivots.shape[0]
    slot_cap = max(16, 2 * piv_count // devices)
    owner = pivots // rows_dev
    counter = jnp.arange(piv_count, dtype=jnp.int32)
    earlier = (counter[None, :] < counter[:, None]) & (owner[None, :] == owner[:, None])
    rank = jnp.sum(earlier, axis=1).astype(jnp.int32)
    target = owner * slot_cap + rank
    vectors = finished.shape[1] // devices
    local = (pivots % rows_dev).astype(jnp.float32)
    received, gathered = exchange(
        mesh_shape, target[None, :], local[None, :], finished, prior, slot_cap
    )
    return finish(
        received, pairs, occupied, panel, prior, gathered.reshape(width, piv_count), vectors
    )


def solution(mesh):
    mesh_shape = (mesh.shape["row"], mesh.shape["col"])
    return jax.shard_map(
        functools.partial(per_device, mesh_shape),
        mesh=mesh,
        in_specs=(
            P(),
            P(("row", "col"), None),
            P(("row", "col"), None),
            P(("row", "col"), None),
            P(),
            P(),
        ),
        out_specs=(P(("row", "col"), None), P(("row", "col"), None, None)),
        check_vma=False,
    )
```
